32 devices in a mesh: row: 16 (over z, y, x), col: 2 (over core).
Axes of the slice: x: 2, y: 2, z: 4, core: 2. Of those that a mesh axis runs over, the one named last changes fastest.
Arguments:
- centroids: float32 [3, 14336], P(None, ('row', 'col')), may hold values from -6 to 6
- normals: float32 [3, 14336], P(None, ('col', 'row')), may hold values from -6 to 6
- nodes: float32 [18, 14336], P(None, ('col', 'row')), may hold values from -6 to 6
- weights: float32 [6, 14336], P(None, ('col', 'row')), may hold values from 0.25 to 1
- row_scale: float32 [14336], P('row'), may hold values from 0.5 to 2
- col_scale: float32 [14336], P('col'), may hold values from 0.5 to 2
Outputs:
- transformed: float32 [14336, 14336], P('row', 'col')
The draws below stay inside these ranges and needn't reach their ends.
All inputs are finite; a program needn't handle non-finite values.
Results may differ from the reference program's by a relative error of at most 0.0003.
Values sent between devices are 32-bit elements; how exact they have to be, the bound alone decides.
A program may use at most 128 MiB of HBM per device.

```python
import math
import jax
import jax.numpy as jnp
from jax import lax

ORDER = 14336
NODES = 6


def level_of(own_key, dims, pieces, low, high):
    level, own = 1.0, jax.random.fold_in(own_key, 6)
    for position, blocks in pieces:
        steps = jnp.exp(jax.random.uniform(jax.random.fold_in(own, position), (blocks,), jnp.float32, low / len(pieces), high / len(pieces)))
        level = level * jnp.repeat(steps, dims[position] // blocks).reshape([-1 if axis == position else 1 for axis in range(len(dims))])
    return level


def noise(stream_key, dims, width, reach, pieces=(), kind=jnp.bfloat16):
    array = width * jax.random.normal(stream_key, dims, jnp.float32)
    if pieces:
        array = array * level_of(stream_key, dims, pieces, -0.22, 0.18)
    return jnp.clip(array, -reach, reach).astype(kind)


def setup_inputs(seed: int = 0) -> dict:
    splits = jax.random.split(jax.random.key(seed), 7)
    centroids = noise(splits[0], (3, ORDER), 1.0, 6.0, ((1, 32),), jnp.float32)
    normals = noise(splits[1], (3, ORDER), 1.0, 6.0, ((1, 32),), jnp.float32)
    nodes = noise(splits[2], (3 * NODES, ORDER), 1.0, 6.0, ((1, 32),), jnp.float32)
    weights = jnp.clip(jnp.exp(math.log(1.0) - 1.3862944 * jax.random.uniform(splits[3], (NODES, ORDER), jnp.float32) ** level_of(splits[3], (NODES, ORDER), ((1, 32),), -0.2, 0.2)), 0.25, 1.0)
    row_scale = jnp.clip(jnp.exp(math.log(2.0) - 1.3862944 * jax.random.uniform(splits[4], (ORDER,), jnp.float32) ** level_of(splits[4], (ORDER,), ((0, 16),), -0.2, 0.2)), 0.5, 2.0)
    col_scale = jnp.clip(jnp.exp(math.log(2.0) - 1.3862944 * jax.random.uniform(splits[5], (ORDER,), jnp.float32) ** level_of(splits[5], (ORDER,), ((0, 2),), -0.2, 0.2)), 0.5, 2.0)
    return dict(centroids=centroids, normals=normals, nodes=nodes, weights=weights, row_scale=row_scale, col_scale=col_scale)


core_square = 0.0625
kernel_scale = 1.0 / (4.0 * math.pi)
butterfly_scale = 1.0 / math.sqrt(2.0)

def assemble(targets, panel_table, row_start, col_start):
    count = (panel_table.shape[0] - 3) // 4
    height = targets.shape[1]
    breadth = panel_table.shape[1]
    total = jnp.zeros((height, breadth), jnp.float32)
    for which in range(count):
        along_x = targets[0][:, None] - panel_table[3 + 3 * which][None, :]
        along_y = targets[1][:, None] - panel_table[4 + 3 * which][None, :]
        along_z = targets[2][:, None] - panel_table[5 + 3 * which][None, :]
        distance = along_x * along_x + along_y * along_y + along_z * along_z + core_square
        normal_dot = panel_table[0][None, :] * along_x + panel_table[1][None, :] * along_y + panel_table[2][None, :] * along_z
        total = total + panel_table[3 + 3 * count + which][None, :] * normal_dot * lax.rsqrt(distance) / distance
    row_ids = row_start + jnp.arange(height, dtype=jnp.int32)
    col_ids = col_start + jnp.arange(breadth, dtype=jnp.int32)
    return total * kernel_scale + jnp.where(row_ids[:, None] == col_ids[None, :], 0.5, 0.0)

def reference(centroids, normals, nodes, weights, row_scale, col_scale):
    panel_table = jnp.concatenate([normals, nodes, weights], 0)
    order = centroids.shape[1]
    half = order // 2
    block = math.gcd(half, 256)
    blocks = half // block

    def one_block(index):
        first = (index * block).astype(jnp.int32)
        second = (first + half).astype(jnp.int32)
        upper_points = lax.dynamic_slice_in_dim(centroids, first, block, 1)
        lower_points = lax.dynamic_slice_in_dim(centroids, second, block, 1)
        upper = assemble(upper_points, panel_table, first, jnp.int32(0))
        lower = assemble(lower_points, panel_table, second, jnp.int32(0))
        upper_gain = lax.dynamic_slice_in_dim(row_scale, first, block, 0)[:, None]
        lower_gain = lax.dynamic_slice_in_dim(row_scale, second, block, 0)[:, None]
        mixed_upper = upper_gain * (upper + lower) * butterfly_scale
        mixed_lower = lower_gain * (upper - lower) * butterfly_scale
        mixed = jnp.stack([mixed_upper, mixed_lower], 0)
        left_gain = col_scale[:half][None, None, :]
        right_gain = col_scale[half:][None, None, :]
        left = left_gain * (mixed[:, :, :half] + mixed[:, :, half:]) * butterfly_scale
        right = right_gain * (mixed[:, :, :half] - mixed[:, :, half:]) * butterfly_scale
        return jnp.concatenate([left, right], 2)
    stacked = lax.map(one_block, jnp.arange(blocks, dtype=jnp.int32))
    return jnp.transpose(stacked, (1, 0, 2, 3)).reshape(order, order)
```

```python
import functools
import math

import jax
import jax.numpy as jnp
from jax import lax
from jax.experimental import pallas as pl
from jax.experimental.pallas import tpu as pltpu
from jax.sharding import PartitionSpec as P

core_square = 0.0625
kernel_scale = 1.0 / (4.0 * math.pi)
MESH = pl.DeviceIdType.MESH
SUB = 32
LIMIT = 60 * 1024 * 1024
SPLITS = (0, 0, 0, 1, 1, 2)
SLOTS = [(piece, axis) for axis in range(4) for piece in SPLITS] + [(0, 4)] * 3


def gather_body(
    rows, cores, normals, nodes, weights, centroids, table, near,
    x_ref, g_ref, send_sem, recv_sem, pass_sem, take_sem,
):
    me = lax.axis_index("row")
    core = lax.axis_index("col")
    side = core // (cores // 2)
    other = lax.rem(core + cores // 2, cores)
    count = weights.shape[0]
    x_ref[...] = jnp.ones_like(x_ref)
    for axis in range(3):
        for which in range(count):
            row = 3 * which + axis
            x_ref[8 * axis + which : 8 * axis + which + 1, :] = nodes[row : row + 1, :]
        x_ref[8 * axis + 6 : 8 * axis + 7, :] = normals[axis : axis + 1, :]
        x_ref[8 * axis + 7 : 8 * axis + 8, :] = centroids[axis : axis + 1, :]
    x_ref[24 : 24 + count, :] = weights[...]

    barrier = pltpu.get_barrier_semaphore()
    for step in range(1, rows):
        pl.semaphore_signal(
            barrier, inc=1, device_id=(lax.rem(me + step, rows), core), device_id_type=MESH
        )
    pl.semaphore_signal(barrier, inc=1, device_id=(me, other), device_id_type=MESH)
    pl.semaphore_wait(barrier, rows)

    sends = []
    for step in range(1, rows):
        copy = pltpu.make_async_remote_copy(
            src_ref=x_ref,
            dst_ref=g_ref.at[me, side],
            send_sem=send_sem.at[step],
            recv_sem=recv_sem.at[step],
            device_id=(lax.rem(me + step, rows), core),
            device_id_type=MESH,
        )
        copy.start()
        sends.append(copy)
    passes = []
    first = pltpu.make_async_remote_copy(
        src_ref=x_ref,
        dst_ref=g_ref.at[me, side],
        send_sem=pass_sem.at[0],
        recv_sem=take_sem.at[0],
        device_id=(me, other),
        device_id_type=MESH,
    )
    first.start()
    passes.append(first)
    g_ref[me, side] = x_ref[...]
    for step in range(1, rows):
        sends[step - 1].wait_recv()
        source = lax.rem(me + rows - step, rows)
        copy = pltpu.make_async_remote_copy(
            src_ref=g_ref.at[source, side],
            dst_ref=g_ref.at[source, side],
            send_sem=pass_sem.at[step],
            recv_sem=take_sem.at[step],
            device_id=(me, other),
            device_id_type=MESH,
        )
        copy.start()
        passes.append(copy)
    for copy in sends:
        copy.wait_send()
    for copy in passes:
        copy.wait()
    width = x_ref.shape[1]
    for part in range(2):
        for source in range(rows):
            start = (part * rows + source) * width
            table[:, start : start + width] = g_ref[source, part]
    low = lax.rem(me, rows // 2)
    for part in range(2):
        for axis in range(3):
            near[part, axis : axis + 1, :] = g_ref[
                low + part * (rows // 2), side, 8 * axis + 7 : 8 * axis + 8, :
            ]


def gather(normals, nodes, weights, centroids):
    rows = lax.axis_size("row")
    cores = lax.axis_size("col")
    width = normals.shape[1]
    return pl.pallas_call(
        functools.partial(gather_body, rows, cores),
        out_shape=[
            jax.ShapeDtypeStruct((32, 2 * rows * width), jnp.float32),
            jax.ShapeDtypeStruct((2, 3, width), jnp.float32),
        ],
        in_specs=[pl.BlockSpec(memory_space=pltpu.VMEM)] * 4,
        out_specs=[pl.BlockSpec(memory_space=pltpu.VMEM)] * 2,
        scratch_shapes=[
            pltpu.VMEM((32, width), jnp.float32),
            pltpu.VMEM((rows, 2, 32, width), jnp.float32),
            pltpu.SemaphoreType.DMA((rows,)),
            pltpu.SemaphoreType.DMA((rows,)),
            pltpu.SemaphoreType.DMA((rows,)),
            pltpu.SemaphoreType.DMA((rows,)),
        ],
        compiler_params=pltpu.CompilerParams(
            collective_id=0, has_side_effects=True, vmem_limit_bytes=LIMIT
        ),
        name="gather",
    )(normals, nodes, weights, centroids)


def pieces(value):
    one = value.astype(jnp.bfloat16).astype(jnp.float32)
    rest = value - one
    two = rest.astype(jnp.bfloat16).astype(jnp.float32)
    return one, two, rest - two


def panel_rows(count, table):
    x, y, z, weight = table[0:8, :], table[8:16, :], table[16:24, :], table[24:32, :]
    row = lax.broadcasted_iota(jnp.int32, x.shape, 0)
    node = row < count
    gain = jnp.where(node, jnp.exp2(jnp.log2(weight) * (-2.0 / 3.0)), 0.0)
    factor = jnp.where(row == 6, kernel_scale, -2.0 * gain)
    level = gain * (x * x + y * y + z * z + core_square)
    parts = []
    for value in (x * factor, y * factor, z * factor, gain):
        one, two, three = pieces(value)
        parts += [one, two, three, one, two, one]
    parts += list(pieces(level))
    parts += [jnp.zeros_like(x)] * (32 - len(parts))
    grid = jnp.concatenate(parts, 0).astype(jnp.bfloat16)
    offset = kernel_scale * (x[6:7, :] * x + y[6:7, :] * y + z[6:7, :] * z)
    return grid, offset


def work_body(
    count, begin, rows, tile, sub, info, near, rowgain, left, right, colgain, *refs
):
    keep, send, points, gain, grid_left, grid_right, off_left, off_right, dot_a, dot_b = refs[-10:]
    row_sign = info[1].astype(jnp.float32)
    col_sign = info[2].astype(jnp.float32)
    first_row = info[3]
    column = pl.program_id(0) * tile
    steps = rows // sub
    span = 2 * sub

    @pl.when(pl.program_id(0) == 0)
    def _():
        group = lax.broadcasted_iota(jnp.int32, (24, 256), 1) // 8
        source = lax.broadcasted_iota(jnp.int32, (24, 256), 0)
        spread = jnp.zeros((24, 256), jnp.float32)
        for slot, (piece, axis) in enumerate(SLOTS):
            spread = jnp.where((group == slot) & (source == 8 * piece + axis), 1.0, spread)
        pick = lax.broadcasted_iota(jnp.int32, (24, 128), 0)
        pick = jnp.where((pick == 5) | (pick == 13) | (pick == 21), 1.0, 0.0)
        lane = lax.broadcasted_iota(jnp.int32, (sub, 256), 1)
        place = lane - (lane // 8) * 8
        for half in range(2):
            x = near[half, 0:1, begin : begin + rows]
            y = near[half, 1:2, begin : begin + rows]
            z = near[half, 2:3, begin : begin + rows]
            own = rowgain[0, 0:1, begin : begin + rows] * 0.5
            zero = jnp.zeros_like(x)
            stack = [x, y, z, x * x + y * y + z * z, zero + 1.0, own, zero, zero]
            three = jnp.concatenate(pieces(jnp.concatenate(stack, 0)), 0)
            flat = jnp.transpose(three, (1, 0)).astype(jnp.bfloat16)
            wide = jnp.dot(
                flat, spread.astype(jnp.bfloat16), preferred_element_type=jnp.float32
            )
            if half == 0:
                gain[...] = jnp.dot(
                    flat, pick.astype(jnp.bfloat16), preferred_element_type=jnp.float32
                )
            for index in range(steps):
                block = wide[index * sub : (index + 1) * sub, :]
                for which in range(count + 1):
                    spot = which if which < count else 6
                    at = which * span + half * sub
                    points[index, at : at + sub, :] = jnp.where(
                        place == spot, block, 0.0
                    ).astype(jnp.bfloat16)

    grid, offset = panel_rows(count, left)
    grid_left[...] = grid
    off_left[...] = offset
    grid, offset = panel_rows(count, right)
    grid_right[...] = grid
    off_right[...] = offset

    def product(index, grid):
        return jnp.dot(points[index], grid[...], preferred_element_type=jnp.float32)

    def mix(dots, off):
        base = dots[count * span : (count + 1) * span, :]
        total = None
        for which in range(count):
            root = lax.rsqrt(dots[which * span : (which + 1) * span, :])
            term = (base - off[which : which + 1, :]) * (root * root * root)
            total = term if total is None else total + term
        return total[:sub] + row_sign * total[sub:]

    dot_a[...] = product(0, grid_left)

    def step(index, carry):
        at = pl.ds(pl.multiple_of(index * sub, sub), sub)
        dot_b[...] = product(index, grid_right)
        lift = gain[at, :]
        lift = jnp.concatenate([lift] * (tile // 128), 1)
        mixed_left = mix(dot_a, off_left) * lift
        dot_a[...] = product(jnp.minimum(index + 1, steps - 1), grid_left)
        mixed_right = mix(dot_b, off_right) * (lift * col_sign)
        keep[at, :] = (mixed_left + mixed_right) * colgain[...]
        send[at, :] = mixed_left - mixed_right
        return carry

    lax.fori_loop(0, steps, step, 0)

    @pl.when((column < first_row + rows) & (column + tile > first_row))
    def _():
        down = lax.broadcasted_iota(jnp.int32, (rows, tile), 0) + first_row
        over = lax.broadcasted_iota(jnp.int32, (rows, tile), 1) + column
        lift = jnp.concatenate([gain[...]] * (tile // 128), 1)
        spot = jnp.where(down == over, 0.5, 0.0) * lift
        turn = row_sign * col_sign
        keep[...] += spot * (1.0 + turn) * colgain[...]
        send[...] += spot * (1.0 - turn)


def work(count, info, near, rowgain, table, colgain, out, height, begin, end):
    rows = end - begin
    half = table.shape[1] // 2
    tile = math.gcd(half, 256)
    tiles = half // tile
    sub = math.gcd(rows, SUB)
    share = near.shape[2]
    lhs = (count + 1) * 2 * sub
    in_specs = [
        pl.BlockSpec((2, 3, share), lambda j, s: (0, 0, 0)),
        pl.BlockSpec((1, 1, share), lambda j, s: (s[4], 0, 0)),
        pl.BlockSpec((32, tile), lambda j, s: (0, j)),
        pl.BlockSpec((32, tile), lambda j, s: (0, j + tiles)),
        pl.BlockSpec((1, tile), lambda j, s: (0, j)),
    ]
    operands = [info, near, rowgain, table, table, colgain]
    alias = {}
    if out is not None:
        in_specs.append(pl.BlockSpec(memory_space=pl.ANY))
        alias = {len(operands): 0}
        operands.append(out)
    return pl.pallas_call(
        functools.partial(work_body, count, begin, rows, tile, sub),
        grid_spec=pltpu.PrefetchScalarGridSpec(
            num_scalar_prefetch=1,
            grid=(tiles,),
            in_specs=in_specs,
            out_specs=[
                pl.BlockSpec(
                    (pl.Element(rows), pl.Element(tile)),
                    lambda j, s: (pl.multiple_of(s[0] * 8, 8), j * tile),
                ),
                pl.BlockSpec((rows, tile), lambda j, s: (0, j)),
            ],
            scratch_shapes=[
                pltpu.VMEM((rows // sub, lhs, 256), jnp.bfloat16),
                pltpu.VMEM((rows, 128), jnp.float32),
                pltpu.VMEM((256, tile), jnp.bfloat16),
                pltpu.VMEM((256, tile), jnp.bfloat16),
                pltpu.VMEM((8, tile), jnp.float32),
                pltpu.VMEM((8, tile), jnp.float32),
                pltpu.VMEM((lhs, tile), jnp.float32),
                pltpu.VMEM((lhs, tile), jnp.float32),
            ],
        ),
        out_shape=[
            jax.ShapeDtypeStruct((height, half), jnp.float32),
            jax.ShapeDtypeStruct((rows, half), jnp.float32),
        ],
        input_output_aliases=alias,
        compiler_params=pltpu.CompilerParams(vmem_limit_bytes=LIMIT),
        cost_estimate=pl.CostEstimate(
            flops=rows * half * 4 * 7 * 512,
            bytes_accessed=rows * half * 8,
            transcendentals=rows * half * 4 * 6,
        ),
        name=f"work_{begin}",
    )(*operands)

def merge_body(info, got, colgain, _, out):
    out[...] = got[...] * colgain[...]


def merge(info, got, colgain, out):
    height, breadth = out.shape
    rows = got.shape[0]
    step = math.gcd(rows, 32)
    return pl.pallas_call(
        merge_body,
        grid_spec=pltpu.PrefetchScalarGridSpec(
            num_scalar_prefetch=1,
            grid=(rows // step,),
            in_specs=[
                pl.BlockSpec((step, breadth), lambda i, s: (i, 0)),
                pl.BlockSpec((1, breadth), lambda i, s: (0, 0)),
                pl.BlockSpec(memory_space=pl.ANY),
            ],
            out_specs=pl.BlockSpec(
                (pl.Element(step), pl.Element(breadth)),
                lambda i, s: (pl.multiple_of(s[0] * 8 + i * step, 8), 0),
            ),
        ),
        out_shape=jax.ShapeDtypeStruct(out.shape, jnp.float32),
        input_output_aliases={3: 0},
        compiler_params=pltpu.CompilerParams(vmem_limit_bytes=LIMIT),
        cost_estimate=pl.CostEstimate(
            flops=rows * breadth, bytes_accessed=rows * breadth * 8, transcendentals=0
        ),
        name="merge",
    )(info, got, colgain, out)


def per_device(centroids, normals, nodes, weights, row_scale, col_scale):
    rows = lax.axis_size("row")
    cores = lax.axis_size("col")
    row_pos = lax.axis_index("row")
    col_pos = lax.axis_index("col")
    half_row = rows // 2
    half_col = cores // 2
    height = row_scale.shape[0]
    breadth = col_scale.shape[0]
    count = weights.shape[0]
    share = height // 2
    table, near = gather(normals, nodes, weights, centroids)

    upper = row_pos < half_row
    low = lax.rem(row_pos, half_row)
    low_col = lax.rem(col_pos, half_col)
    core = col_pos // half_col
    if cores > 2:
        mine = lax.all_gather(centroids, "col", axis=1, tiled=True)
        hops = [(source, (source + half_row) % rows) for source in range(rows)]
        far = lax.ppermute(mine, "row", hops)
        near = jnp.stack([jnp.where(upper, mine, far), jnp.where(upper, far, mine)], 0)
        near = lax.dynamic_slice_in_dim(near, core * share, share, 2)
    rowgain = row_scale.reshape(2, 1, share)
    colgain = col_scale[None, :]

    unit = math.gcd(share, 64)
    blocks = share // unit
    front = (blocks * 4 + 6) // 7
    cuts = [(0, front * unit), (front * unit, share)]
    row_sign = jnp.where(upper, 1, -1)
    col_sign = jnp.where(core == 0, 1, -1)
    swap = [(source, (source + half_col) % cores) for source in range(cores)]
    out = None
    got = []
    for begin, end in cuts:
        where = core * share + begin
        first_row = low * height + where - low_col * breadth
        info = jnp.stack([where // 8, row_sign, col_sign, first_row, core]).astype(jnp.int32)
        out, send = work(
            count, info, near, rowgain, table, colgain, out, height, begin, end
        )
        got.append(lax.ppermute(send, "col", swap))
    for (begin, end), block in zip(cuts, got):
        where = (1 - core) * share + begin
        info = jnp.stack([where // 8]).astype(jnp.int32)
        out = merge(info, block, colgain, out)
    return out


def solution(mesh):
    placed = (
        P(None, ("row", "col")),
        P(None, ("col", "row")),
        P(None, ("col", "row")),
        P(None, ("col", "row")),
        P("row"),
        P("col"),
    )
    return jax.shard_map(
        per_device, mesh=mesh, in_specs=placed, out_specs=P("row", "col"), check_vma=False
    )
```
